32 devices in a mesh: seq: 8 (over y, x, core), head: 4 (over z).
Axes of the slice: x: 2, y: 2, z: 4, core: 2. Of those that a mesh axis runs over, the one named last changes fastest.
Arguments:
- query_raw: float32 [2048, 16, 128], P('seq', 'head'), may hold values from -150 to 150
- key_raw: float32 [2048, 16, 128], P('seq', 'head'), may hold values from -150 to 150
- value_raw: float32 [2048, 16, 128], P('seq', 'head'), may hold values from -6 to 6
- query_gain: float32 [16, 128], P('head'), may hold values from 0.25 to 1.75
- key_gain: float32 [16, 128], P('head'), may hold values from 0.25 to 1.75
- cotangent: float32 [2048, 16, 128], P('seq', 'head'), may hold values from -6 to 6
Outputs:
- attended: float32 [2048, 16, 128], P('seq', 'head')
- grad_query: float32 [2048, 16, 128], P('seq', 'head')
- grad_key: float32 [2048, 16, 128], P('seq', 'head')
- grad_value: float32 [2048, 16, 128], P('seq', 'head')
The draws below stay inside these ranges and needn't reach their ends.
All inputs are finite; a program needn't handle non-finite values.
Results may differ from the reference program's by a relative error of at most 0.00023.
Values sent between devices are 32-bit elements; how exact they have to be, the bound alone decides.
No kernel may reach another device: no remote copies, remote signals or barrier semaphores. Data moves between devices by JAX's collectives and lax.ppermute only.
A program may use at most 64 MiB of HBM per device.

```python
import jax
import jax.numpy as jnp
from jax import lax

DK = 128
TOK_DEV = 256
HEADS = 16
TOKENS = 2048
N_SEQ = 8


def draw_scaled(key, salt):
    key = jax.random.fold_in(key, salt)
    first, second = jax.random.split(key, 2)
    channel = jnp.exp(jax.random.uniform(first, (HEADS, DK), jnp.float32) * jnp.log(10.0))
    ramp = jnp.exp(jnp.log(3.0) * jnp.arange(HEADS).astype(jnp.float32) / max(HEADS - 1, 1))
    base = jnp.clip(jax.random.normal(second, (TOKENS, HEADS, DK), jnp.float32), -5.0, 5.0)
    return (base * channel[None] * ramp[None, :, None]).astype(jnp.float32)


def draw_query_raw(key, part):
    return draw_scaled(key, 11)


def draw_key_raw(key, part):
    return draw_scaled(key, 23)


def shard_levels(key, shape, cuts, least, top_value):
    loudness, own = 1.0, jax.random.fold_in(key, 6)
    for axis_at, blocks in cuts:
        heights = jnp.exp(jax.random.uniform(jax.random.fold_in(own, axis_at), (blocks,), jnp.float32, least / len(cuts), top_value / len(cuts)))
        loudness = loudness * jnp.repeat(heights, shape[axis_at] // blocks).reshape([-1 if axis == axis_at else 1 for axis in range(len(shape))])
    return loudness


def centred(rng, dims, spread, limit, cuts=(), held_as=jnp.bfloat16):
    drawn = spread * jax.random.normal(rng, dims, jnp.float32)
    if cuts:
        drawn = drawn * shard_levels(rng, dims, cuts, -0.22, 0.18)
    return jnp.clip(drawn, -limit, limit).astype(held_as)


def setup_inputs(seed: int = 0) -> dict:
    seeds = jax.random.split(jax.random.key(seed), 7)
    return {
        "query_raw": draw_query_raw(jax.random.fold_in(seeds[6], 71), 0),
        "key_raw": draw_key_raw(jax.random.fold_in(seeds[6], 71), 0),
        "value_raw": centred(seeds[2], (TOKENS, HEADS, DK), 1.0, 6.0, ((0, 8), (1, 4)), jnp.float32),
        "query_gain": jnp.clip(1.0 + 0.15 * jax.random.normal(seeds[3], (HEADS, DK), jnp.float32), 0.25, 1.75),
        "key_gain": jnp.clip(1.0 + 0.15 * jax.random.normal(seeds[4], (HEADS, DK), jnp.float32), 0.25, 1.75),
        "cotangent": centred(seeds[5], (TOKENS, HEADS, DK), 1.0, 6.0, ((0, 8), (1, 4)), jnp.float32),
    }


epsilon = 1e-06
highest = lax.Precision.HIGHEST

def product(form, left, right):
    return jnp.einsum(form, left, right, precision=highest)

def normalize(raw, gain):
    scale = lax.rsqrt(lax.optimization_barrier(jnp.mean(raw * raw, axis=(1, 2), keepdims=True)) + epsilon)
    return raw * scale * gain[None]

def layer(query_in, key_in, value_in, query_gain, key_gain):
    query_hat = normalize(query_in, query_gain)
    key_hat = normalize(key_in, key_gain)
    query_blocks = query_hat.reshape(N_SEQ, TOK_DEV, HEADS, DK)
    key_blocks = key_hat.reshape(N_SEQ, TOK_DEV, HEADS, DK)
    value_blocks = value_in.reshape(N_SEQ, TOK_DEV, HEADS, DK)
    indices = jnp.arange(TOK_DEV)
    causal = indices[:, None] >= indices[None, :]

    def advance(state, blocks):
        query_blk, key_blk, value_blk = blocks
        scores = jnp.where(causal[None], product('thd,shd->hts', query_blk, key_blk), 0.0)
        result = product('hts,she->the', scores, value_blk) + product('thd,hde->the', query_blk, state)
        state = state + product('thd,the->hde', key_blk, value_blk)
        return (state, result)
    initial = jnp.zeros((HEADS, DK, DK), jnp.float32)
    _, outputs = lax.scan(jax.checkpoint(advance), initial, (query_blocks, key_blocks, value_blocks))
    position = jnp.arange(TOKENS).astype(jnp.float32)
    weight = lax.rsqrt(DK * (position + 1.0))
    return outputs.reshape(TOKENS, HEADS, DK) * weight[:, None, None]

def reference(query_raw, key_raw, value_raw, query_gain, key_gain, cotangent):

    def forward_only(query_in, key_in, value_in):
        return layer(query_in, key_in, value_in, query_gain, key_gain)
    attended, pullback = jax.vjp(forward_only, query_raw, key_raw, value_raw)
    grad_query, grad_key, grad_value = pullback(cotangent)
    return (attended, grad_query, grad_key, grad_value)
```

```python
import functools

import jax
import jax.numpy as jnp
from jax import lax
from jax.experimental import pallas as pl
from jax.experimental.pallas import tpu as pltpu
from jax.sharding import PartitionSpec as P

epsilon = 1e-06
wide = jnp.float32
half_type = jnp.bfloat16
cores = 2
vmem_bytes = 12 * 1024 * 1024


def split(value):
    high = value.astype(half_type)
    low = (value - high.astype(wide)).astype(half_type)
    return high, low


def dot(left, right, left_dim=1, right_dim=0):
    return lax.dot_general(
        left, right, (((left_dim,), (right_dim,)), ((), ())), preferred_element_type=wide
    )


def row_sums(value):
    high, low = split(value)
    ones = jnp.ones((8, value.shape[1]), half_type)
    return (dot(ones, high, 1, 1) + dot(ones, low, 1, 1))[0:1]


def column_of(row):
    return jnp.transpose(jnp.broadcast_to(row, (8, row.shape[1])))[:, 0:1]


def head_rows(ref, head, heads):
    return ref[pl.ds(head, ref.shape[0] // heads, stride=heads), :]


def weight_column(place, tokens, head_size):
    index = lax.broadcasted_iota(jnp.int32, (tokens, head_size), 0)
    position = (place * tokens + index).astype(wide)
    return lax.rsqrt(float(head_size) * (position + 1.0))


def squares_kernel(heads, query_ref, key_ref, out_ref):
    for at, ref in enumerate((query_ref, key_ref)):
        total = None
        for head in range(heads):
            rows = head_rows(ref, head, heads)
            total = rows * rows if total is None else total + rows * rows
        out_ref[at : at + 1, :] = row_sums(total)


def prepare_kernel(
    heads, axis, query_ref, key_ref, value_ref, cot_ref, query_gain_ref, key_gain_ref,
    query_t_ref, key_t_ref, value_two_ref, cot_two_ref,
    score_high_ref, score_low_ref, mix_high_ref, mix_low_ref,
):
    tokens = query_ref.shape[0] // heads
    size = query_ref.shape[1]
    weight = weight_column(lax.axis_index(axis), tokens, size)
    causal = lax.broadcasted_iota(jnp.int32, (tokens, tokens), 0) >= lax.broadcasted_iota(
        jnp.int32, (tokens, tokens), 1
    )
    for head in range(heads):
        query = head_rows(query_ref, head, heads) * query_gain_ref[head : head + 1, :]
        key = head_rows(key_ref, head, heads) * key_gain_ref[head : head + 1, :]
        value = head_rows(value_ref, head, heads)
        cot = head_rows(cot_ref, head, heads) * weight
        query_t_ref[head] = jnp.transpose(query)
        key_t_ref[head] = jnp.transpose(key)
        for left, right, two_ref, high_ref, low_ref in (
            (query, key, None, score_high_ref, score_low_ref),
            (cot, value, None, mix_high_ref, mix_low_ref),
        ):
            left_high, left_low = split(left)
            right_high, right_low = split(right)
            if high_ref is mix_high_ref:
                cot_two_ref[head, :, :size] = left_high
                cot_two_ref[head, :, size:] = left_low
                value_two_ref[head, :, :size] = right_high
                value_two_ref[head, :, size:] = right_low
            product = dot(
                jnp.concatenate([left_high, left_low], 1),
                jnp.concatenate([right_high, right_high], 1), 1, 1,
            ) + dot(left_high, right_low, 1, 1)
            high, low = split(jnp.where(causal, product, 0.0))
            high_ref[head] = high
            low_ref[head] = low


def states_kernel(heads, width, *refs):
    *part_refs, query_t_ref, key_t_ref, value_two_ref, cot_two_ref, scale_ref, state_ref, grad_ref = refs
    size = query_t_ref.shape[1]
    total = part_refs[0][...]
    for ref in part_refs[1:]:
        total = total + ref[...]
    scale = lax.rsqrt(total * (1.0 / width) + epsilon)
    scale_ref[...] = scale
    for raw_ref, row, other_ref, out_ref in (
        (key_t_ref, scale[1:2], value_two_ref, state_ref),
        (query_t_ref, scale[0:1], cot_two_ref, grad_ref),
    ):
        for head in range(heads):
            high, low = split(raw_ref[head] * row)
            pair = dot(jnp.concatenate([high, low], 0), other_ref[head])
            out_ref[head * size : (head + 1) * size, :] = (
                pair[:size, :size] + pair[:size, size:] + pair[size:, :size]
            )


def intra_kernel(
    heads, scale_ref, query_ref, key_ref, query_gain_ref, key_gain_ref, value_two_ref, cot_two_ref,
    score_high_ref, score_low_ref, mix_high_ref, mix_low_ref,
    query_two_ref, key_two_ref, attended_ref, grad_query_ref, grad_key_ref, grad_value_ref,
):
    size = query_ref.shape[1]
    query_scale = column_of(scale_ref[0:1, :])
    key_scale = column_of(scale_ref[1:2, :])

    def by_two(high, low, right, transposed):
        right_high, right_low = split(right)
        dim = 0 if transposed else 1
        both = dot(high, jnp.concatenate([right_high, right_low], 1), dim, 0)
        return both[:, :size] + both[:, size:] + dot(low, right_high, dim, 0)

    for head in range(heads):
        query = head_rows(query_ref, head, heads) * query_gain_ref[head : head + 1, :] * query_scale
        key = head_rows(key_ref, head, heads) * key_gain_ref[head : head + 1, :] * key_scale
        value = value_two_ref[head, :, :size].astype(wide) + value_two_ref[head, :, size:].astype(wide)
        cot = cot_two_ref[head, :, :size].astype(wide) + cot_two_ref[head, :, size:].astype(wide)
        for source, ref in ((query, query_two_ref), (key, key_two_ref)):
            high, low = split(source)
            ref[head, :, :size] = high
            ref[head, :, size:] = low
        score_high, score_low = score_high_ref[head], score_low_ref[head]
        mix_high, mix_low = mix_high_ref[head], mix_low_ref[head]
        attended_ref[head] = by_two(score_high, score_low, value * key_scale, False) * query_scale
        grad_value_ref[head] = by_two(score_high, score_low, cot * query_scale, True) * key_scale
        grad_query_ref[head] = by_two(mix_high, mix_low, key, False)
        grad_key_ref[head] = by_two(mix_high, mix_low, query, True)


def outputs_kernel(
    heads, axis, earlier_ref, later_ref, query_two_ref, key_two_ref, attended_in_ref, grad_value_in_ref,
    value_ref, cot_ref, attended_ref, grad_value_ref, inner_ref,
):
    tokens = value_ref.shape[0] // heads
    size = value_ref.shape[1]
    weight = weight_column(lax.axis_index(axis), tokens, size)
    blank = jnp.zeros((size, size), half_type)
    for at, (state_ref, two_ref, intra_ref, other_ref, out_ref) in enumerate((
        (earlier_ref, query_two_ref, attended_in_ref, cot_ref, attended_ref),
        (later_ref, key_two_ref, grad_value_in_ref, value_ref, grad_value_ref),
    )):
        inner = None
        for head in range(heads):
            high, low = split(state_ref[head * size : (head + 1) * size, :])
            right = jnp.concatenate(
                [jnp.concatenate([high, low], 1), jnp.concatenate([high, blank], 1)], 0
            )
            both = dot(two_ref[head], right)
            result = both[:, :size] + both[:, size:] + intra_ref[head]
            if at == 0:
                result = result * weight
            out_ref[pl.ds(head, tokens, stride=heads), :] = result
            term = result * head_rows(other_ref, head, heads)
            inner = term if inner is None else inner + term
        inner_ref[at : at + 1, :] = row_sums(inner)


def pushes_kernel(
    heads, scale_ref, earlier_ref, later_ref, cot_two_ref, value_two_ref, grad_query_ref, grad_key_ref,
    query_gain_ref, key_gain_ref, query_push_ref, key_push_ref,
):
    tokens = cot_two_ref.shape[1]
    size = query_gain_ref.shape[1]
    blank = jnp.zeros((size, size), half_type)
    for at, (state_ref, two_ref, intra_ref, gain_ref, out_ref) in enumerate((
        (earlier_ref, cot_two_ref, grad_query_ref, query_gain_ref, query_push_ref),
        (later_ref, value_two_ref, grad_key_ref, key_gain_ref, key_push_ref),
    )):
        scale = column_of(scale_ref[at : at + 1, :])
        for head in range(heads):
            high, low = split(state_ref[head * size : (head + 1) * size, :])
            right = jnp.concatenate(
                [jnp.concatenate([high, high], 1), jnp.concatenate([low, blank], 1)], 0
            )
            both = dot(two_ref[head], right, 1, 1)
            result = (both[:, :size] + both[:, size:] + intra_ref[head]) * gain_ref[head : head + 1, :]
            out_ref[pl.ds(head, tokens, stride=heads), :] = result * scale


def final_kernel(heads, width, *refs):
    *part_refs, scale_ref, query_ref, key_ref, query_push_ref, key_push_ref, query_out_ref, key_out_ref = refs
    tokens = query_ref.shape[0] // heads
    total = part_refs[0][...]
    for ref in part_refs[1:]:
        total = total + ref[...]
    factor = scale_ref[...] * scale_ref[...] * total * (1.0 / width)
    for at, (raw_ref, push_ref, out_ref) in enumerate((
        (query_ref, query_push_ref, query_out_ref),
        (key_ref, key_push_ref, key_out_ref),
    )):
        column = column_of(factor[at : at + 1])
        for head in range(heads):
            out_ref[pl.ds(head, tokens, stride=heads), :] = head_rows(
                push_ref, head, heads
            ) - head_rows(raw_ref, head, heads) * column


def call(kernel, outs, args, flops, name):
    whole = pl.BlockSpec(memory_space=pltpu.VMEM)
    shapes = [jax.ShapeDtypeStruct(shape, kind) for shape, kind in outs]
    moved = sum(a.size * a.dtype.itemsize for a in (*args, *shapes))
    return pl.pallas_call(
        kernel,
        out_shape=shapes,
        in_specs=[whole] * len(args),
        out_specs=[whole] * len(shapes),
        compiler_params=pltpu.CompilerParams(vmem_limit_bytes=vmem_bytes),
        cost_estimate=pl.CostEstimate(flops=int(flops), bytes_accessed=int(moved), transcendentals=0),
        name=name,
    )(*args)


def from_others(part, axis):
    count = lax.axis_size(axis)
    paired = count & (count - 1) == 0
    parts = [part]
    for step in range(count - 1, 0, -1):
        pairs = [(at, at ^ step if paired else (at + step) % count) for at in range(count)]
        parts.append(lax.ppermute(part, axis, pairs))
    return parts


def radices(count):
    out = []
    while count % 4 == 0 and count > 1:
        out.append(4)
        count //= 4
    divisor = 2
    while count > 1:
        while count % divisor == 0:
            out.append(divisor)
            count //= divisor
        divisor += 1
    return out


def neighbour_states(state, grad, axis):
    count = lax.axis_size(axis)
    place = lax.axis_index(axis)
    swap = [(at, at ^ 1) for at in range(count)]
    core = place % cores
    other_state = lax.ppermute(state, axis, swap)
    other_grad = lax.ppermute(grad, axis, swap)
    rows = state.shape[0] // cores

    def mine(value):
        return lax.dynamic_slice_in_dim(value, core * rows, rows, 0)

    up = mine(state) + mine(other_state)
    down = mine(grad) + mine(other_grad)
    earlier = jnp.zeros_like(up)
    later = jnp.zeros_like(down)
    stride = cores
    steps = radices(count // cores)
    for level, radix in enumerate(steps):
        last = level == len(steps) - 1
        paired = radix & (radix - 1) == 0
        digit = place // stride % radix
        got = []
        for step in range(1, radix):
            pairs = []
            for at in range(count):
                own = at // stride % radix
                goal = own ^ step if paired else (own + step) % radix
                pairs.append((at, at + (goal - own) * stride))
            target = digit ^ step if paired else (digit + step) % radix
            source = digit ^ step if paired else (digit + radix - step) % radix
            if last:
                message = jnp.where(target > digit, up, down)
            else:
                message = jnp.concatenate([up, down], 0)
            got.append((source, lax.ppermute(message, axis, pairs)))
        for source, message in got:
            first, second = (message, message) if last else (message[:rows], message[rows:])
            earlier = earlier + jnp.where(source < digit, first, 0.0)
            later = later + jnp.where(source > digit, second, 0.0)
            if not last:
                up = up + first
                down = down + second
        stride *= radix
    both = jnp.concatenate([earlier, later], 0)
    shared = lax.ppermute(both, axis, swap)

    def whole(own, shared_part):
        return jnp.where(
            core == 0,
            jnp.concatenate([own, shared_part], 0),
            jnp.concatenate([shared_part, own], 0),
        )

    return (
        whole(earlier, shared[:rows]) + jnp.where(core == 1, other_state, 0.0),
        whole(later, shared[rows:]) + jnp.where(core == 0, other_grad, 0.0),
    )


def local(query_raw, key_raw, value_raw, query_gain, key_gain, cotangent):
    tokens, heads, size = query_raw.shape
    width = float(heads * size * lax.axis_size("head"))
    query, key, value, cot = (
        a.reshape(tokens * heads, size) for a in (query_raw, key_raw, value_raw, cotangent)
    )
    rows = ((2, tokens), wide)
    flat = ((tokens * heads, size), wide)
    square = ((heads, tokens, tokens), half_type)
    twice = ((heads, tokens, 2 * size), half_type)
    turned = ((heads, size, tokens), wide)
    stack = ((heads, tokens, size), wide)
    state_shape = ((heads * size, size), wide)
    work = 2 * heads * tokens * tokens * size

    (squares,) = call(functools.partial(squares_kernel, heads), [rows], [query, key], work / 8, "squares")
    parts = from_others(squares, "head")
    query_t, key_t, value_two, cot_two, *grids = call(
        functools.partial(prepare_kernel, heads, "seq"),
        [turned, turned, twice, twice, square, square, square, square],
        [query, key, value, cot, query_gain, key_gain], 6 * work, "prepare",
    )
    scale, state, grad = call(
        functools.partial(states_kernel, heads, width), [rows, state_shape, state_shape],
        [*parts, query_t, key_t, value_two, cot_two], 4 * work, "states",
    )
    query_two, key_two, attended_in, grad_query_in, grad_key_in, grad_value_in = call(
        functools.partial(intra_kernel, heads),
        [twice, twice, stack, stack, stack, stack],
        [scale, query, key, query_gain, key_gain, value_two, cot_two, *grids], 12 * work, "intra",
    )
    earlier, later = neighbour_states(state, grad, "seq")
    attended, grad_value, inner = call(
        functools.partial(outputs_kernel, heads, "seq"), [flat, flat, rows],
        [earlier, later, query_two, key_two, attended_in, grad_value_in, value, cot], 4 * work, "outputs",
    )
    inners = from_others(inner, "head")
    query_push, key_push = call(
        functools.partial(pushes_kernel, heads), [flat, flat],
        [scale, earlier, later, cot_two, value_two, grad_query_in, grad_key_in, query_gain, key_gain],
        4 * work, "pushes",
    )
    grad_query, grad_key = call(
        functools.partial(final_kernel, heads, width), [flat, flat],
        [*inners, scale, query, key, query_push, key_push], work / 8, "final",
    )
    return tuple(
        a.reshape(tokens, heads, size) for a in (attended, grad_query, grad_key, grad_value)
    )


def solution(mesh):
    tensor = P("seq", "head", None)
    gain = P("head", None)
    return jax.shard_map(
        local,
        mesh=mesh,
        in_specs=(tensor, tensor, tensor, gain, gain, tensor),
        out_specs=(tensor,) * 4,
        check_vma=False,
    )
```
